128 devices in a mesh: ctx: 16 (over x, z_hi, core), exp: 8 (over y, z_lo).
Axes of the slice: x: 4, y: 4, z: 4 (z_hi: 2, z_lo: 2; z = z_hi * 2 + z_lo), core: 2. Of those that a mesh axis runs over, the one named last changes fastest.
Arguments:
- query: bfloat16 [2048, 4096], P('ctx', 'exp'), may hold values from -8 to 8
- keys_values: bfloat16 [2, 2048, 1024], P(None, 'ctx', 'exp'), may hold values from -8 to 8
- cache: bfloat16 [2, 4096, 1024], P(None, 'ctx', 'exp'), may hold values from -8 to 8
- residual: bfloat16 [2048, 4096], P(('ctx', 'exp')), may hold values from -6 to 6
- out_proj: bfloat16 [4096, 4096], P('exp'), may hold values from -0.09375 to 0.09375
- norm_gain: float32 [4096], replicated, may hold values from 0.1 to 1.9
- router: bfloat16 [4096, 8], replicated, may hold values from -0.09375 to 0.09375
- expert_ids: int32 [2048, 2], P(('ctx', 'exp')), may hold values from 0 to 7, all different within a row; in each aligned block of 16 rows (0 to 15, 16 to 31, ...) at most 8 rows name the same one
- w_gate: bfloat16 [8, 4096, 8192], P('exp', None, 'ctx'), may hold values from -0.09375 to 0.09375
- w_up: bfloat16 [8, 4096, 8192], P('exp', None, 'ctx'), may hold values from -0.09375 to 0.09375
- w_down: bfloat16 [8, 8192, 4096], P('exp', 'ctx'), may hold values from -0.0625 to 0.0625
- cotangent: bfloat16 [2048, 4096], P(('ctx', 'exp')), may hold values from -6 to 6
Outputs:
- layer_out: bfloat16 [2048, 4096], P(('ctx', 'exp'))
- grad_down: float32 [8, 8192, 4096], P('exp', 'ctx')
The draws below stay inside these ranges and needn't reach their ends.
Inputs may be any that keep to these rules, and one draw needn't show every extreme that they name: `expert_ids`: each row names two different experts. Within each aligned block of 16 rows no expert is named by more than 8 rows.
All inputs are finite; a program needn't handle non-finite values.
Results may differ from the reference program's by a relative error of at most 0.012.
Values may be sent and summed in bfloat16 or wider, within the bound.
A program may use at most 128 MiB of HBM per device.

```python
import math
import jax
import jax.numpy as jnp
import numpy as np
from jax import lax

D = 4096
QUERY_HEADS = 32
KEY_VALUE_HEADS = 8
HEAD_SIZE = 128
FF = 8192
WINDOW = 4096
EXPERTS = 8
NEW_TOKENS = 2048
CACHED_TOKENS = 4096
ROWS_DEV = 16
CAP = 8
N_CTX = 16
N_EXP = 8


def drawn_pair(key):
    base = jax.random.fold_in(key, 101)
    key_query, key_index_pairs = jax.random.split(base, 2)
    queries = jax.random.normal(key_query, (NEW_TOKENS, QUERY_HEADS * HEAD_SIZE), jnp.float32)
    index_pairs = jax.random.normal(key_index_pairs, (2, NEW_TOKENS, KEY_VALUE_HEADS * HEAD_SIZE), jnp.float32)
    return (jnp.clip(queries, -8.0, 8.0), jnp.clip(index_pairs, -8.0, 8.0))


def draw_query(key, part):
    return drawn_pair(key)[0].astype(jnp.bfloat16)


def draw_keys_values(key, part):
    return drawn_pair(key)[1].astype(jnp.bfloat16)


def shard_levels(rng, dims, cuts, least, high):
    loudness, own = 1.0, jax.random.fold_in(rng, 6)
    for axis_at, shards_of in cuts:
        steps = jnp.exp(jax.random.uniform(jax.random.fold_in(own, axis_at), (shards_of,), jnp.float32, least / len(cuts), high / len(cuts)))
        loudness = loudness * jnp.repeat(steps, dims[axis_at] // shards_of).reshape([-1 if axis == axis_at else 1 for axis in range(len(dims))])
    return loudness


def routed_block(stream_key, own, number, rows, amount, top, reach, slope):
    order = jax.random.permutation(stream_key, amount)
    crowded, ordinary = load_shares(amount, rows * top, reach, slope, True), load_shares(amount, rows * top, reach, slope, False)
    places = jnp.arange(amount)

    def named(sizes, turn):
        used = int((sizes > 0).sum())
        fixed = max(1, used // 4)
        moved = fixed + (places - fixed + turn * (used - fixed)) % max(1, amount - fixed)
        return jnp.zeros((amount,), jnp.int32).at[order[jnp.where(places < fixed, places, moved)]].set(jnp.asarray(sizes, jnp.int32))

    sizes = jnp.where(number % 4 == 0, named(crowded, number // 4), named(ordinary, number - number // 4 - 1))
    mixed = jax.random.permutation(jax.random.fold_in(own, 3), amount)
    source_of, sink = mixed[0:amount // 2 * 2:2], mixed[1:amount // 2 * 2:2]
    margin = jnp.minimum(sizes[source_of] - 1, reach - sizes[sink]) // 2
    margin = jnp.where((source_of == order[0]) | (sink == order[0]) | (sizes[sink] == 0), 0, jnp.maximum(margin, 0))
    moved = jax.random.randint(jax.random.fold_in(own, 4), (amount // 2,), 0, 1 << 20) % (margin + 1)
    sizes = sizes.at[source_of].add(-moved).at[sink].add(moved)
    items = jnp.searchsorted(jnp.cumsum(sizes), jnp.arange(rows * top), side="right").astype(jnp.int32)
    grid = items.reshape(top, rows).T
    grid = grid[jax.random.permutation(jax.random.fold_in(own, 1), rows)]
    turn = jax.random.randint(jax.random.fold_in(own, 2), (rows, 1), 0, top)
    return jnp.take_along_axis(grid, (jnp.arange(top)[None, :] + turn) % top, axis=1)


def load_shares(count, total, reach, lean, full):
    portions = [(1 << 20) // math.isqrt(rank ** lean) + 1 for rank in range(1, count + 1)]
    largest = reach if full else min(reach, max(-(-total // count), total * portions[0] // sum(portions)))
    least = 1 if total - largest >= count - 1 else 0
    holding, rest = [largest] + [least] * (count - 1), total - largest - least * (count - 1)
    while rest > 0:
        free = [i for i in range(1, count) if holding[i] < largest] or [i for i in range(1, count) if holding[i] < reach]
        whole, budget = sum([portions[i] for i in free]), rest
        for i in free:
            more = min(reach - holding[i], max(1, budget * portions[i] // whole), rest)
            holding[i] = holding[i] + more
            rest = rest - more
    return np.array(holding)


def scatter_about(rng, extent, spread, reach, pieces=(), kind=jnp.bfloat16):
    values = jax.random.normal(rng, extent, jnp.float32) * spread
    if len(pieces) > 0:
        values = shard_levels(rng, extent, pieces, -0.22, 0.18) * values
    return jnp.clip(values, min=-reach, max=reach).astype(kind)


def setup_inputs(seed: int = 0) -> dict:
    arg_keys = jax.random.split(jax.random.key(seed), 13)
    query = draw_query(jax.random.fold_in(arg_keys[12], 71), 0)
    keys_values = draw_keys_values(jax.random.fold_in(arg_keys[12], 71), 0)
    cache = scatter_about(arg_keys[2], (2, CACHED_TOKENS, KEY_VALUE_HEADS * HEAD_SIZE), 1.0, 8.0, ((1, 16), (2, 8)))
    residual = scatter_about(arg_keys[3], (NEW_TOKENS, D), 1.0, 6.0, ((0, 128),))
    out_proj = scatter_about(arg_keys[4], (QUERY_HEADS * HEAD_SIZE, D), (QUERY_HEADS * HEAD_SIZE) ** -0.5, 0.09375, ((0, 8),))
    norm_gain = jnp.clip(1.0 + 0.18 * jax.random.normal(arg_keys[5], (D,), jnp.float32), 0.1, 1.9)
    router = scatter_about(arg_keys[6], (D, EXPERTS), D ** -0.5, 0.09375)
    expert_ids_keys = jax.random.split(jax.random.fold_in(arg_keys[7], 1), NEW_TOKENS // ROWS_DEV)
    expert_ids_turns = jax.random.permutation(jax.random.fold_in(arg_keys[7], 3), NEW_TOKENS // ROWS_DEV)
    expert_ids = jax.vmap(lambda own, number: routed_block(jax.random.fold_in(arg_keys[7], 2), own, number, ROWS_DEV, EXPERTS, 2, CAP, 2))(expert_ids_keys, expert_ids_turns).reshape((NEW_TOKENS, 2))
    w_gate = scatter_about(arg_keys[8], (EXPERTS, D, FF), D ** -0.5, 0.09375, ((0, 8), (2, 16)))
    w_up = scatter_about(arg_keys[9], (EXPERTS, D, FF), D ** -0.5, 0.09375, ((0, 8), (2, 16)))
    w_down = scatter_about(arg_keys[10], (EXPERTS, FF, D), FF ** -0.5, 0.0625, ((0, 8), (1, 16)))
    cotangent = scatter_about(arg_keys[11], (NEW_TOKENS, D), 1.0, 6.0, ((0, 128),))
    return {"query": query, "keys_values": keys_values, "cache": cache, "residual": residual, "out_proj": out_proj, "norm_gain": norm_gain, "router": router, "expert_ids": expert_ids, "w_gate": w_gate, "w_up": w_up, "w_down": w_down, "cotangent": cotangent}


def reference(query, keys_values, cache, residual, out_proj, norm_gain, router, expert_ids, w_gate, w_up, w_down, cotangent):
    head_groups = QUERY_HEADS // KEY_VALUE_HEADS
    query_pos = CACHED_TOKENS + jnp.arange(NEW_TOKENS, dtype=jnp.int32)
    key_pos = jnp.arange(CACHED_TOKENS + NEW_TOKENS, dtype=jnp.int32)
    visible = (key_pos[None, :] <= query_pos[:, None]) & (key_pos[None, :] > query_pos[:, None] - WINDOW)
    key_all = jnp.concatenate([cache[0], keys_values[0]], axis=0)
    value_all = jnp.concatenate([cache[1], keys_values[1]], axis=0)
    score_scale = 1.0 / math.sqrt(HEAD_SIZE)

    def single_head(head_index):
        head_index = head_index.astype(jnp.int32)
        queries = lax.dynamic_slice_in_dim(query, head_index * head_groups * HEAD_SIZE, head_groups * HEAD_SIZE, 1).astype(jnp.float32).reshape(NEW_TOKENS, head_groups, HEAD_SIZE)
        key_rows = lax.dynamic_slice_in_dim(key_all, head_index * HEAD_SIZE, HEAD_SIZE, 1).astype(jnp.float32)
        value_rows = lax.dynamic_slice_in_dim(value_all, head_index * HEAD_SIZE, HEAD_SIZE, 1).astype(jnp.float32)
        scores = jnp.einsum('tjd,kd->tjk', queries, key_rows) * score_scale
        scores = jnp.where(visible[:, None, :], scores, -1e+30)
        row_max = lax.optimization_barrier(jnp.max(scores, axis=-1))
        weights = jnp.where(visible[:, None, :], jnp.exp(scores - row_max[..., None]), 0.0)
        total = lax.optimization_barrier(jnp.sum(weights, axis=-1))
        rounded = lax.optimization_barrier(weights.astype(jnp.bfloat16)).astype(jnp.float32)
        mixed = jnp.einsum('tjk,kd->tjd', rounded, value_rows) / total[..., None]
        return mixed.reshape(NEW_TOKENS, head_groups * HEAD_SIZE)
    per_head_outputs = lax.map(single_head, jnp.arange(KEY_VALUE_HEADS, dtype=jnp.int32))
    attn = jnp.transpose(per_head_outputs, (1, 0, 2)).reshape(NEW_TOKENS, QUERY_HEADS * HEAD_SIZE).astype(jnp.bfloat16)
    hidden_one = residual.astype(jnp.float32) + jnp.dot(attn, out_proj, preferred_element_type=jnp.float32)
    mean_square = lax.optimization_barrier(jnp.mean(hidden_one * hidden_one, axis=-1, keepdims=True))
    normed = (hidden_one * lax.rsqrt(mean_square + 1e-05) * norm_gain).astype(jnp.bfloat16)
    logits = jnp.dot(normed, router, preferred_element_type=jnp.float32)
    onehot = (expert_ids[:, :, None] == jnp.arange(EXPERTS, dtype=jnp.int32)[None, None, :]).astype(jnp.float32)
    chosen = lax.optimization_barrier(jnp.sum(onehot * logits[:, None, :], axis=-1))
    first = 1.0 / (1.0 + jnp.exp(chosen[:, 1] - chosen[:, 0]))
    gates = jnp.stack([first, 1.0 - first], axis=1)
    weight_te = lax.optimization_barrier(jnp.sum(gates[:, :, None] * onehot, axis=1))
    member = lax.optimization_barrier(jnp.sum(onehot, axis=1))
    most_rows = N_CTX * N_EXP * CAP
    group_width = FF // N_CTX
    token_index = jnp.arange(NEW_TOKENS, dtype=jnp.int32)

    def one_expert(combined, inputs):
        gate_mat, up_mat, down_mat, expert_index = inputs
        member_col = jnp.take(member, expert_index, axis=1)
        weight_col = jnp.take(weight_te, expert_index, axis=1)
        keyed = jnp.where(member_col > 0, token_index, NEW_TOKENS + token_index)
        order = jnp.argsort(keyed)[:most_rows].astype(jnp.int32)
        valid = member_col[order]
        rows = jnp.where(valid[:, None] > 0, normed[order], jnp.zeros((), jnp.bfloat16))
        gate_val = jnp.dot(rows, gate_mat, preferred_element_type=jnp.float32)
        up_val = jnp.dot(rows, up_mat, preferred_element_type=jnp.float32)
        hidden_e = (jax.nn.silu(gate_val) * up_val).astype(jnp.bfloat16)
        split_hidden = hidden_e.astype(jnp.float32).reshape(most_rows, N_CTX, group_width)
        split_down = down_mat.astype(jnp.float32).reshape(N_CTX, group_width, D)
        parts = jnp.einsum('rcf,cfd->rcd', split_hidden, split_down)
        parts = lax.optimization_barrier(parts.astype(jnp.bfloat16)).astype(jnp.float32)
        expert_out = lax.optimization_barrier(jnp.sum(parts, axis=1)).astype(jnp.bfloat16).astype(jnp.float32)
        row_weight = weight_col[order] * valid
        combined = combined.at[order].add(row_weight[:, None] * expert_out)
        scaled = (row_weight[:, None] * cotangent[order].astype(jnp.float32)).astype(jnp.bfloat16)
        grad_e = jnp.dot(hidden_e.T, scaled, preferred_element_type=jnp.float32)
        return (combined, grad_e)
    start_sum = jnp.zeros((NEW_TOKENS, D), jnp.float32)
    combined, grad_down = lax.scan(one_expert, start_sum, (w_gate, w_up, w_down, jnp.arange(EXPERTS, dtype=jnp.int32)))
    layer_out = (hidden_one + combined).astype(jnp.bfloat16)
    return (layer_out, grad_down)
```

```python
import functools
import math

import jax
import jax.numpy as jnp
from jax import lax
from jax.experimental import pallas as pl
from jax.experimental.pallas import tpu as pltpu
from jax.sharding import PartitionSpec as P

QUERY_HEADS = 32
KEY_VALUE_HEADS = 8
HEAD_SIZE = 128
WINDOW = 4096
MESH = pl.DeviceIdType.MESH
N_CTX = 16
N_EXP = 8
D = 4096
GROUPS = QUERY_HEADS // KEY_VALUE_HEADS
TOKENS = 128
PRIOR = 256
KEYS = PRIOR + TOKENS
ROWS = 16
CAP = 8
SLOTS = N_EXP * CAP
SCALE = 1.0 / math.sqrt(HEAD_SIZE)
BF16 = jnp.bfloat16
F32 = jnp.float32

epsilon = 1e-05

COPIES = {
    0: (0, 0, "P", None),
    1: (0, 0, "Z", None),
    2: (0, 0, "R", None),
    3: (0, 0, "L", None),
    4: (0, 1, "P", None),
    5: (0, 1, "R", None),
    6: (0, 1, "L", None),
    7: (-1, 0, "P", None),
    8: (-1, 0, "R", 0),
    9: (1, 0, "P", None),
    10: (1, 0, "L", 1),
    11: (2, 0, "P", None),
    12: (-1, 1, "P", None),
    13: (-1, 1, "R", 0),
    14: (1, 1, "P", None),
    15: (1, 1, "L", 1),
    16: (2, 1, "P", None),
}


class Place:
    def __init__(self):
        self.c = lax.axis_index("ctx")
        self.e = lax.axis_index("exp")
        self.x = self.c // 4
        self.z = (self.c // 2) % 2
        self.k = self.c % 2

    def block(self, dx, dz, dk=0):
        return ((self.x + dx + 4) % 4) * 4 + ((self.z + dz) % 2) * 2 + (self.k + dk) % 2

    def peer(self, to):
        at = {"P": (0, 0, 1), "Z": (0, 1, 0), "R": (1, 0, 0), "L": (-1, 0, 0)}[to]
        return (self.block(*at), self.e)

    def expert(self, by):
        return (self.e + by) % N_EXP


class Gather:
    def __init__(self, place, part_of, send, recv):
        self.p, self.part_of, self.send, self.recv = place, part_of, send, recv

    def copy(self, i, arriving):
        dx, dz, to, half = COPIES[i]
        dk = 0
        if arriving:
            if to == "P":
                dk = 1
            elif to == "Z":
                dz = 1 - dz
            elif to == "R":
                dx = dx - 1
            else:
                dx = dx + 1
        ref = self.part_of(self.p.block(dx, dz, dk), half)
        return pltpu.make_async_remote_copy(
            src_ref=ref,
            dst_ref=ref,
            send_sem=self.send.at[i],
            recv_sem=self.recv.at[i],
            device_id=self.p.peer(to),
            device_id_type=MESH,
        )

    def start(self, *ids):
        for i in ids:
            self.copy(i, False).start()

    def wait(self, *ids):
        for i in ids:
            self.copy(i, True).wait_recv()

    def drain(self):
        for i in COPIES:
            self.copy(i, False).wait_send()


def greet(place):
    barrier = pltpu.get_barrier_semaphore()
    peers = [place.peer(to) for to in ("P", "Z", "R", "L")]
    peers += [(place.c, place.expert(j)) for j in range(1, N_EXP)]
    for peer in peers:
        pl.semaphore_signal(barrier, inc=1, device_id=peer, device_id_type=MESH)
    pl.semaphore_wait(barrier, len(peers))


def attention_kernel(
    q_ref, kv_hbm, cache_hbm, w_hbm, cot_ref,
    out_ref, cot_out,
    kv, w, cot, attn, peak, total, mixed, parts, arrived,
    local, kv_send, kv_recv, cot_send, cot_recv, to_send, to_recv, sum_send, sum_recv, put,
):
    place = Place()
    c, e = place.c, place.e
    mine = pl.ds(pl.multiple_of(e * CAP, CAP), CAP)
    loads = [
        pltpu.make_async_copy(cache_hbm, kv.at[c, :, pl.ds(0, PRIOR)], local.at[0]),
        pltpu.make_async_copy(kv_hbm, kv.at[c, :, pl.ds(PRIOR, TOKENS)], local.at[1]),
        pltpu.make_async_copy(cot_ref.at[e], cot.at[c, mine], local.at[2]),
        pltpu.make_async_copy(w_hbm, w, local.at[3]),
    ]
    for load in loads:
        load.start()
    greet(place)

    def kv_part(b, half):
        return kv.at[b] if half is None else kv.at[b, half]

    def cot_part(b, half):
        return cot.at[b] if half is None else cot.at[b, pl.ds(half * 32, 32)]

    keys = Gather(place, kv_part, kv_send, kv_recv)
    cots = Gather(place, cot_part, cot_send, cot_recv)

    def to_expert(j, arriving):
        if arriving:
            at = pl.ds(pl.multiple_of(place.expert(N_EXP - j) * CAP, CAP), CAP)
        else:
            at = mine
        return pltpu.make_async_remote_copy(
            src_ref=cot_ref.at[place.expert(j)],
            dst_ref=cot.at[c, at],
            send_sem=to_send.at[j],
            recv_sem=to_recv.at[j],
            device_id=(c, place.expert(j)),
            device_id_type=MESH,
        )

    loads[0].wait()
    loads[1].wait()
    keys.start(1, 2, 3, 0)
    for j in range(1, N_EXP):
        to_expert(j, False).start()

    peak[...] = jnp.full(peak.shape, -1e30, F32)
    total[...] = jnp.zeros(total.shape, F32)
    mixed[...] = jnp.zeros(mixed.shape, F32)
    token = c * TOKENS + lax.broadcasted_iota(jnp.int32, (TOKENS, 1), 0)

    def attend(dx):
        first = place.block(dx, 0) // 4 * 4
        lane = lax.broadcasted_iota(jnp.int32, (1, 4 * KEYS), 1)
        number = (
            (lane >= KEYS).astype(jnp.int32)
            + (lane >= 2 * KEYS).astype(jnp.int32)
            + (lane >= 3 * KEYS).astype(jnp.int32)
        )
        inside = lane - number * KEYS
        owner = first + number
        old = inside < PRIOR
        below = jnp.where(old, owner * PRIOR + inside, 1 << 30)
        above = jnp.where(old, -1, owner * TOKENS + inside - PRIOR)
        visible = (token < below) & (token >= above)
        offset = jnp.where(visible, 0.0, -1e30)

        @pl.loop(0, GROUPS)
        def _(h):
            key_rows = kv[pl.ds(first, 4), 0].reshape(4 * KEYS, HEAD_SIZE)
            value_rows = kv[pl.ds(first, 4), 1].reshape(4 * KEYS, HEAD_SIZE)
            scores = lax.dot_general(
                q_ref[h], key_rows, (((1,), (1,)), ((), ())), preferred_element_type=F32
            )
            scores = scores * SCALE + offset
            old_peak = peak[h][:, :1]
            new_peak = jnp.maximum(old_peak, jnp.max(scores, axis=-1, keepdims=True))
            weights = jnp.exp(scores - new_peak)
            rescale = jnp.exp(old_peak - new_peak)
            sums = total[h][:, :1] * rescale + jnp.sum(weights, axis=-1, keepdims=True)
            peak[h] = jnp.broadcast_to(new_peak, (TOKENS, HEAD_SIZE))
            total[h] = jnp.broadcast_to(sums, (TOKENS, HEAD_SIZE))
            mixed[h] = mixed[h] * rescale + jnp.dot(
                weights.astype(BF16), value_rows, preferred_element_type=F32
            )

    keys.wait(0, 2)
    keys.start(8, 7)
    keys.wait(3)
    keys.start(10, 9)
    keys.wait(1)
    keys.start(5, 6, 4)
    loads[2].wait()
    for j in range(1, N_EXP):
        to_expert(j, True).wait_recv()
    cots.start(1, 2, 3, 0)
    keys.wait(4)
    attend(0)
    keys.wait(5)
    keys.start(13, 12)
    keys.wait(6)
    keys.start(15, 14)
    keys.wait(8, 10)
    keys.start(11)
    keys.wait(7, 12)
    attend(-1)
    keys.wait(9, 14)
    keys.wait(13, 15)
    keys.start(16)
    attend(1)
    cots.wait(0, 2)
    cots.start(8, 7)
    cots.wait(3)
    cots.start(10, 9)
    keys.wait(11, 16)
    attend(2)

    for h in range(GROUPS):
        attn[:, h * HEAD_SIZE : (h + 1) * HEAD_SIZE] = (mixed[h] / total[h]).astype(BF16)
    loads[3].wait()

    @pl.loop(0, 8)
    def _(n):
        at = pl.ds(pl.multiple_of(n * 512, 512), 512)
        tile = jnp.dot(attn[...], w[:, at], preferred_element_type=F32)
        parts[:, :, at] = tile.astype(BF16).reshape(N_EXP, ROWS, 512)

    def to_owner(j, arriving):
        return pltpu.make_async_remote_copy(
            src_ref=parts.at[place.expert(j)],
            dst_ref=arrived.at[place.expert(N_EXP - j) if arriving else e],
            send_sem=sum_send.at[j],
            recv_sem=sum_recv.at[j],
            device_id=(c, place.expert(j)),
            device_id_type=MESH,
        )

    for j in range(1, N_EXP):
        to_owner(j, False).start()
    cots.wait(1)
    cots.start(5, 6, 4)
    cots.wait(8, 10)
    cots.start(11)
    for j in range(1, N_EXP):
        to_owner(j, True).wait_recv()

    @pl.loop(0, 8)
    def _(n):
        at = pl.ds(pl.multiple_of(n * 512, 512), 512)
        acc = parts[e, :, at].astype(F32)
        for j in range(1, N_EXP):
            acc = acc + arrived[place.expert(j), :, at].astype(F32)
        out_ref[:, at] = acc

    cots.wait(5)
    cots.start(13, 12)
    cots.wait(6)
    cots.start(15, 14)
    cots.wait(13, 15)
    cots.start(16)
    cots.wait(4, 7, 9, 11, 12, 14, 16)
    stores = [pltpu.make_async_copy(cot, cot_out, put)]
    for store in stores:
        store.start()
    for store in stores:
        store.wait()
    keys.drain()
    cots.drain()
    for j in range(1, N_EXP):
        to_expert(j, False).wait_send()
        to_owner(j, False).wait_send()


def attend_and_project(query, keys_values, cache, out_proj, cot_slots):
    queries = jnp.transpose(query.reshape(TOKENS, GROUPS, HEAD_SIZE), (1, 0, 2))
    hbm = pl.BlockSpec(memory_space=pl.ANY)
    vmem = pl.BlockSpec(memory_space=pltpu.VMEM)
    dma = pltpu.SemaphoreType.DMA
    n = len(COPIES)
    return pl.pallas_call(
        attention_kernel,
        out_shape=(
            jax.ShapeDtypeStruct((ROWS, D), F32),
            jax.ShapeDtypeStruct((N_CTX, SLOTS, D), BF16),
        ),
        in_specs=[vmem, hbm, hbm, hbm, vmem],
        out_specs=(vmem, hbm),
        scratch_shapes=[
            pltpu.VMEM((N_CTX, 2, KEYS, HEAD_SIZE), BF16),
            pltpu.VMEM((GROUPS * HEAD_SIZE, D), BF16),
            pltpu.VMEM((N_CTX, SLOTS, D), BF16),
            pltpu.VMEM((TOKENS, GROUPS * HEAD_SIZE), BF16),
            pltpu.VMEM((GROUPS, TOKENS, HEAD_SIZE), F32),
            pltpu.VMEM((GROUPS, TOKENS, HEAD_SIZE), F32),
            pltpu.VMEM((GROUPS, TOKENS, HEAD_SIZE), F32),
            pltpu.VMEM((N_EXP, ROWS, D), BF16),
            pltpu.VMEM((N_EXP, ROWS, D), BF16),
            dma((4,)),
            dma((n,)),
            dma((n,)),
            dma((n,)),
            dma((n,)),
            dma((N_EXP,)),
            dma((N_EXP,)),
            dma((N_EXP,)),
            dma((N_EXP,)),
            dma,
        ],
        compiler_params=pltpu.CompilerParams(
            collective_id=0, has_side_effects=True, vmem_limit_bytes=48 * 1024 * 1024
        ),
        name="attention_kernel",
    )(queries, keys_values, cache, out_proj, cot_slots)


def experts_part(outgoing, weighted_rows, cot_all, gate_mat, up_mat, down_mat, hidden_one):
    gate_col = jnp.sum(weighted_rows, axis=-1, keepdims=True)
    high = gate_col.astype(BF16)
    low = (gate_col - high.astype(F32)).astype(BF16)
    extra = jnp.concatenate([high, low, jnp.zeros((SLOTS, 126), BF16)], axis=1)
    both = jnp.concatenate([outgoing, extra], axis=1).reshape(N_EXP, CAP, D + 128)
    arrived = lax.all_to_all(both, "exp", split_axis=0, concat_axis=0, tiled=True)
    rows_all = lax.all_gather(arrived.reshape(SLOTS, D + 128), "ctx", axis=0, tiled=True)
    gate_all = rows_all[:, D].astype(F32) + rows_all[:, D + 1].astype(F32)
    rows_all = rows_all[:, :D]
    gate_val = jnp.dot(rows_all, gate_mat, preferred_element_type=F32)
    up_val = jnp.dot(rows_all, up_mat, preferred_element_type=F32)
    hidden_all = (jax.nn.silu(gate_val) * up_val).astype(BF16)
    expert_out = lax.psum_scatter(
        jnp.dot(hidden_all, down_mat, preferred_element_type=F32).astype(BF16),
        "ctx",
        scatter_dimension=0,
        tiled=True,
    )
    returned = lax.all_to_all(
        expert_out.reshape(N_EXP, CAP, D), "exp", split_axis=0, concat_axis=0, tiled=True
    )
    combined = jnp.dot(weighted_rows.T, returned.reshape(SLOTS, D).astype(F32))
    layer_out = (hidden_one + combined).astype(BF16)
    gated = (gate_all[:, None] * hidden_all.astype(F32)).astype(BF16)
    gradient = lax.dot_general(
        gated, cot_all.reshape(N_CTX * SLOTS, D), (((0,), (0,)), ((), ())), preferred_element_type=F32
    )
    return (layer_out, gradient[None])


def on_device(
    query,
    keys_values,
    cache,
    residual,
    out_proj,
    norm_gain,
    router,
    expert_ids,
    w_gate,
    w_up,
    w_down,
    cotangent,
):
    experts = router.shape[1]
    onehot = (expert_ids[:, :, None] == jnp.arange(experts, dtype=jnp.int32)[None, None, :]).astype(F32)
    assigned = ROWS * 2
    flat_hot = onehot.reshape(assigned, experts)
    earlier = (jnp.arange(assigned)[:, None] > jnp.arange(assigned)[None, :]).astype(F32)
    before = jnp.dot(earlier, flat_hot)
    slot = jnp.sum(before * flat_hot, axis=-1).astype(jnp.int32)
    target = expert_ids.reshape(assigned) * CAP + slot
    dispatch = (jnp.arange(SLOTS, dtype=jnp.int32)[:, None] == target[None, :]).astype(F32)
    dispatch = dispatch.reshape(SLOTS, ROWS, 2)
    pick_rows = jnp.sum(dispatch, axis=-1)
    picks = pick_rows.astype(BF16)
    cot_slots = jnp.dot(picks, cotangent, preferred_element_type=F32).astype(BF16)
    cot_slots = cot_slots.reshape(experts, CAP, D)

    projected, cot_all = attend_and_project(query, keys_values, cache, out_proj, cot_slots)

    hidden_one = residual.astype(F32) + projected
    mean_square = jnp.mean(hidden_one * hidden_one, axis=-1, keepdims=True)
    normed = (hidden_one * lax.rsqrt(mean_square + epsilon) * norm_gain).astype(BF16)
    logits = jnp.dot(normed, router, preferred_element_type=F32)
    chosen = jnp.sum(onehot * logits[:, None, :], axis=-1)
    first = 1.0 / (1.0 + jnp.exp(chosen[:, 1] - chosen[:, 0]))
    gates = jnp.stack([first, 1.0 - first], axis=1)
    weighted_rows = jnp.sum(dispatch * gates[None, :, :], axis=-1)
    outgoing = jnp.dot(picks, normed, preferred_element_type=F32).astype(BF16)
    return experts_part(
        outgoing, weighted_rows, cot_all, w_gate[0], w_up[0], w_down[0], hidden_one
    )


def solution(mesh):
    placed = (
        P("ctx", "exp"),
        P(None, "ctx", "exp"),
        P(None, "ctx", "exp"),
        P(("ctx", "exp"), None),
        P("exp", None),
        P(),
        P(),
        P(("ctx", "exp"), None),
        P("exp", None, "ctx"),
        P("exp", None, "ctx"),
        P("exp", "ctx", None),
        P(("ctx", "exp"), None),
    )
    return jax.shard_map(
        on_device,
        mesh=mesh,
        in_specs=placed,
        out_specs=(P(("ctx", "exp"), None), P("exp", "ctx", None)),
        check_vma=False,
    )
```
